32 devices in a mesh: rows: 8 (over z, y), cols: 4 (over x, core).
Axes of the slice: x: 2, y: 2, z: 4, core: 2. Of those that a mesh axis runs over, the one named last changes fastest.
Arguments:
- matrix: bfloat16 [2048, 8192], P('rows', 'cols'), may hold values from -0.125 to 0.125
- inverse: bfloat16 [16384, 8192], P('rows', 'cols'), may hold values from -1 to 1
- target: float32 [2048, 128], P('rows'), may hold values from -60 to 60
- penalty: float32 [128], replicated, may hold values from 0.5 to 16
- consensus: float32 [8192, 128], P('cols'), may hold values from -6 to 6
- copy_duals: float32 [8, 8192, 128], P('rows', 'cols'), may hold values from -6 to 6
- fit_parts: float32 [4, 2048, 128], P('cols', 'rows'), may hold values from -6 to 6
- fit_mean: float32 [2048, 128], P('rows'), may hold values from -3 to 3
- fit_duals: float32 [2048, 128], P('rows'), may hold values from -3 to 3
Outputs:
- coefficients: float32 [8192, 128], P('cols')
- fitted: float32 [2048, 128], P('rows')
- history: float32 [5, 2], replicated
The draws below stay inside these ranges and needn't reach their ends.
All inputs are finite; a program needn't handle non-finite values.
Results may differ from the reference program's by a relative error of at most 0.006.
Values sent between devices are 32-bit elements; how exact they have to be, the bound alone decides.
No kernel may reach another device: no remote copies, remote signals or barrier semaphores. Data moves between devices by JAX's collectives and lax.ppermute only.
A program may use at most 64 MiB of HBM per device.

```python
import math
import jax
import jax.numpy as jnp
from jax import lax

COLS_DEV = 2048
ROWS_DEV = 256
TARGETS = 128
ITERS = 5
ALL_ROWS = 2048
ALL_COLS = 8192
N_ROWS = 8
N_COLS = 4


def draw_inverse(key, part):
    noise_key, scale_key = jax.random.split(jax.random.fold_in(key, 11))
    shape = (N_ROWS, COLS_DEV, N_COLS, COLS_DEV)
    entries = jax.random.normal(noise_key, shape, jnp.float32)
    levels = jax.random.uniform(scale_key, (N_ROWS, COLS_DEV, N_COLS, 1), jnp.float32, 0.5, 1.0)
    entries = jnp.clip(entries, -6.0, 6.0) * (0.2 / math.sqrt(COLS_DEV))
    identity = jnp.eye(COLS_DEV, dtype=jnp.float32)[None, :, None, :]
    result = entries * (1.0 - identity) + identity * levels
    return result.reshape(N_ROWS * COLS_DEV, N_COLS * COLS_DEV).astype(jnp.bfloat16)


def draw_target(key, part):
    noise_key = jax.random.fold_in(jax.random.fold_in(key, 23), 0)
    rising = jnp.power(3.0, jnp.arange(ALL_ROWS, dtype=jnp.float32) / ALL_ROWS)
    values = jax.random.truncated_normal(noise_key, -6.0, 6.0, (ALL_ROWS, TARGETS), jnp.float32)
    return values * rising[:, None]


def block_levels(stream_key, shape, pieces, smallest, high):
    level, own = 1.0, jax.random.fold_in(stream_key, 6)
    for dim, blocks in pieces:
        steps = jnp.exp(jax.random.uniform(jax.random.fold_in(own, dim), (blocks,), jnp.float32, smallest / len(pieces), high / len(pieces)))
        level = level * jnp.repeat(steps, shape[dim] // blocks).reshape([-1 if axis == dim else 1 for axis in range(len(shape))])
    return level


def noise(rng, extent, scale, bound, pieces=(), kind=jnp.bfloat16):
    values = scale * jax.random.normal(rng, extent, jnp.float32)
    if pieces:
        values = values * block_levels(rng, extent, pieces, -0.22, 0.18)
    return jnp.clip(values, -bound, bound).astype(kind)


def setup_inputs(seed: int = 0) -> dict:
    key_list = jax.random.split(jax.random.key(seed), 10)
    return {
        "matrix": noise(key_list[0], (ALL_ROWS, ALL_COLS), COLS_DEV ** -0.5, 0.125, ((0, 8), (1, 4))),
        "inverse": draw_inverse(jax.random.fold_in(key_list[9], 71), 0),
        "target": draw_target(jax.random.fold_in(key_list[9], 71), 0),
        "penalty": jnp.clip(jnp.exp(jax.random.uniform(key_list[3], (TARGETS,), jnp.float32, math.log(0.5), math.log(16.0))), 0.5, 16.0),
        "consensus": noise(key_list[4], (ALL_COLS, TARGETS), 1.0, 6.0, ((0, 4),), jnp.float32),
        "copy_duals": noise(key_list[5], (N_ROWS, ALL_COLS, TARGETS), 0.5, 6.0, ((0, 8), (1, 4)), jnp.float32),
        "fit_parts": noise(key_list[6], (N_COLS, ALL_ROWS, TARGETS), 1.0, 6.0, ((0, 4), (1, 8)), jnp.float32),
        "fit_mean": noise(key_list[7], (ALL_ROWS, TARGETS), 0.2, 3.0, ((0, 8),), jnp.float32),
        "fit_duals": noise(key_list[8], (ALL_ROWS, TARGETS), 0.2, 3.0, ((0, 8),), jnp.float32),
    }


def reference(matrix, inverse, target, penalty, consensus, copy_duals, fit_parts, fit_mean, fit_duals):
    blocks = matrix.reshape(N_ROWS, ROWS_DEV, N_COLS, COLS_DEV)
    caches = inverse.reshape(N_ROWS, COLS_DEV, N_COLS, COLS_DEV)
    center = consensus.reshape(N_COLS, COLS_DEV, TARGETS)
    duals = copy_duals.reshape(N_ROWS, N_COLS, COLS_DEV, TARGETS)
    shares = jnp.transpose(fit_parts.reshape(N_COLS, N_ROWS, ROWS_DEV, TARGETS), (1, 0, 2, 3))
    observed = target.reshape(N_ROWS, ROWS_DEV, TARGETS)
    fitted_mean = fit_mean.reshape(N_ROWS, ROWS_DEV, TARGETS)
    row_dual = fit_duals.reshape(N_ROWS, ROWS_DEV, TARGETS)
    threshold = penalty / N_ROWS
    normalizer = N_ROWS * ALL_COLS * TARGETS
    mean_share = jnp.sum(shares, axis=1) / N_COLS
    records = []
    for iteration in range(ITERS):
        offsets = (shares - mean_share[:, None] + fitted_mean[:, None] - row_dual[:, None]).astype(jnp.bfloat16)

        def project(operands):
            tile_rows, cached, offset_row, dual_row = operands
            tile_float = tile_rows.astype(jnp.float32)
            pulled = jnp.einsum("rjc,jrt->jct", tile_float, offset_row.astype(jnp.float32))
            right_side = lax.optimization_barrier((center - dual_row + pulled).astype(jnp.bfloat16))
            copies = jnp.einsum("cjd,jdt->jct", cached.astype(jnp.float32), right_side.astype(jnp.float32))
            rounded = lax.optimization_barrier(copies.astype(jnp.bfloat16))
            fresh_shares = jnp.einsum("rjc,jct->jrt", tile_float, rounded.astype(jnp.float32))
            return copies, fresh_shares

        copies, shares = lax.map(project, (blocks, caches, offsets, duals))
        mean_share = jnp.sum(shares, axis=1) / N_COLS
        average = jnp.sum(copies + duals, axis=0) / N_ROWS
        updated = average - jnp.clip(average, -threshold, threshold)
        motion = N_ROWS * jnp.sum((updated - center) ** 2)
        center = updated
        fitted_mean = (observed + row_dual + mean_share) / (N_COLS + 1)
        spread = jnp.sum((copies - center[None]) ** 2) + N_COLS * jnp.sum((mean_share - fitted_mean) ** 2)
        records.append(jnp.stack([spread, motion]) / normalizer)
        duals = duals + copies - center[None]
        row_dual = row_dual + mean_share - fitted_mean
    history = jnp.stack(records)
    return center.reshape(ALL_COLS, TARGETS), (fitted_mean * N_COLS).reshape(ALL_ROWS, TARGETS), history
```

```python
import jax
import jax.numpy as jnp
from jax import lax
from jax.sharding import PartitionSpec as P

ITERS = 5


def shrink(values, cutoff):
    return values - jnp.clip(values, -cutoff, cutoff)


def swap(values, axis, size, bit):
    return lax.ppermute(values, axis, [(i, i ^ bit) for i in range(size)])


def butterfly(values, axis, bits, size):
    for bit in bits:
        values = values + swap(values, axis, size, bit)
    return values


def bits_of(size):
    bits, bit = [], 1
    while bit < size:
        bits.append(bit)
        bit *= 2
    return bits


def halve(parts, bits, index, size):
    for step in range(len(bits[0])):
        sent = []
        kept = []
        for part, order in zip(parts, bits):
            bit = order[step]
            low, high = jnp.split(part, 2, axis=0)
            upper = (index & bit) != 0
            kept.append(jnp.where(upper, high, low))
            sent.append(swap(jnp.where(upper, low, high), "rows", size, bit))
        parts = [k + s for k, s in zip(kept, sent)]
    return parts


def double(parts, bits, index, size):
    for step in reversed(range(len(bits[0]))):
        got = [swap(part, "rows", size, order[step]) for part, order in zip(parts, bits)]
        joined = []
        for part, other, order in zip(parts, got, bits):
            upper = (index & order[step]) != 0
            joined.append(
                jnp.concatenate([jnp.where(upper, other, part), jnp.where(upper, part, other)], axis=0)
            )
        parts = joined
    return parts


def local(matrix, inverse, target, penalty, consensus, copy_duals, fit_parts, fit_mean, fit_duals):
    row_devices = lax.axis_size("rows")
    col_devices = lax.axis_size("cols")
    index = lax.axis_index("rows")
    block_width, targets = consensus.shape
    normalizer = float(row_devices * col_devices * block_width * targets)
    threshold = penalty / row_devices
    row_bits, col_bits = bits_of(row_devices), bits_of(col_devices)
    orders = [row_bits, row_bits[1:] + row_bits[:1]]
    cut = block_width // 2
    copy_dual = copy_duals[0]
    shares = fit_parts[0]
    mean_share = butterfly(shares, "cols", col_bits, col_devices) / col_devices
    center = consensus
    fitted_mean = fit_mean
    row_dual = fit_duals
    records = []
    for iteration in range(ITERS):
        offsets = (shares - mean_share + fitted_mean - row_dual).astype(jnp.bfloat16)
        pulled = lax.dot_general(
            matrix, offsets, (((0,), (0,)), ((), ())), preferred_element_type=jnp.float32
        )
        right_side = (center - copy_dual + pulled).astype(jnp.bfloat16)
        copies = jnp.dot(inverse, right_side, preferred_element_type=jnp.float32)
        shares = jnp.dot(matrix, copies.astype(jnp.bfloat16), preferred_element_type=jnp.float32)
        mean_share = butterfly(shares, "cols", col_bits, col_devices) / col_devices
        summed_in = copies + copy_dual
        sums = halve([summed_in[:cut], summed_in[cut:]], orders, index, row_devices)
        owned = [shrink(s / row_devices, threshold) for s in sums]
        updated = jnp.concatenate(double(owned, orders, index, row_devices), axis=0)
        motion = jnp.sum((updated - center) ** 2)
        center = updated
        fitted_mean = (target + row_dual + mean_share) / (col_devices + 1)
        spread = jnp.sum((copies - center) ** 2) + jnp.sum((mean_share - fitted_mean) ** 2)
        records.append(jnp.stack([spread, motion]))
        if iteration + 1 < ITERS:
            copy_dual = copy_dual + copies - center
            row_dual = row_dual + mean_share - fitted_mean
    history = jnp.stack(records)
    history = butterfly(history, "cols", col_bits, col_devices)
    history = butterfly(history, "rows", row_bits, row_devices) / normalizer
    return (center, fitted_mean * col_devices, history)


def solution(mesh):
    in_specs = (
        P("rows", "cols"),
        P("rows", "cols"),
        P("rows", None),
        P(),
        P("cols", None),
        P("rows", "cols", None),
        P("cols", "rows", None),
        P("rows", None),
        P("rows", None),
    )
    out_specs = (P("cols", None), P("rows", None), P())
    return jax.shard_map(local, mesh=mesh, in_specs=in_specs, out_specs=out_specs, check_vma=False)
```

```python
import functools

import jax
import jax.numpy as jnp
from jax import lax
from jax.experimental import pallas as pl
from jax.experimental.pallas import tpu as pltpu
from jax.sharding import PartitionSpec as P

ITERS = 5
STREAMS = 4
F32 = jnp.float32
BF16 = jnp.bfloat16


def bits_of(size):
    bits, bit = [], 1
    while bit < size:
        bits.append(bit)
        bit *= 2
    return bits


def swap(values, axis, size, bit):
    return lax.ppermute(values, axis, [(i, i ^ bit) for i in range(size)])


def butterfly(values, axis, size):
    for bit in bits_of(size):
        values = values + swap(values, axis, size, bit)
    return values


def fold(values):
    squares = values * values
    return jnp.sum(squares.reshape(-1, 8, squares.shape[-1]), axis=0)


def dot(a, b):
    return jnp.dot(a, b, preferred_element_type=F32)


def call(body, outs, *args, scratch=(), flops=0):
    return pl.pallas_call(
        body,
        out_shape=[jax.ShapeDtypeStruct(s, d) for s, d in outs],
        scratch_shapes=list(scratch),
        cost_estimate=pl.CostEstimate(flops=flops * 8, bytes_accessed=0, transcendentals=0),
        compiler_params=pltpu.CompilerParams(vmem_limit_bytes=8 * 1024 * 1024),
    )(*args)


def first_offsets(cols, shares, total, fitted_mean, row_dual, tall, out):
    offsets = shares[...] - total[...] / cols + fitted_mean[...] - row_dual[...]
    out[...] = dot(tall[...], offsets.astype(BF16))


def next_offsets(cols, slot, shares, total, target, row_dual, tall, log, out, dual_out, log_out):
    mean_share = total[...] / cols
    fitted_mean = (target[...] + row_dual[...] + mean_share) / (cols + 1)
    dual = row_dual[...] + mean_share - fitted_mean
    offsets = shares[...] - mean_share + fitted_mean - dual
    out[...] = dot(tall[...], offsets.astype(BF16))
    dual_out[...] = dual
    log_out[...] = log[...]
    log_out[slot : slot + 8] += fold(mean_share - fitted_mean)


def last_fit(cols, slot, total, target, row_dual, log, out, log_out):
    mean_share = total[...] / cols
    fitted_mean = (target[...] + row_dual[...] + mean_share) / (cols + 1)
    out[...] = fitted_mean * cols
    log_out[...] = log[...]
    log_out[slot : slot + 8] += fold(mean_share - fitted_mean)


def first_copies(inverse, center, copy_dual, pulled, copies, *sums):
    right_side = (center[...] - copy_dual[...] + pulled[...]).astype(BF16)
    rows = right_side.shape[0] // len(sums)
    for n, out in enumerate(sums):
        part = slice(n * rows, (n + 1) * rows)
        made = dot(inverse[part, :], right_side)
        copies[part, :] = made
        out[...] = made + copy_dual[part, :]


def update(n, slot, total, plain, inverse, new, old, copies, copy_dual, pulled, log, *rest):
    rows = new.shape[0]
    part = slice(n * rows, (n + 1) * rows)
    gap = copies[part, :] - new[...]
    dual = copy_dual[...] + gap
    right_side = (new[...] - dual + pulled[part, :]).astype(BF16)
    if n == 0:
        dual_out, log_out, out = rest
        out[...] = dot(inverse[:, part], right_side)
    elif n < total - 1:
        begun, dual_out, log_out, out = rest
        out[...] = begun[...] + dot(inverse[:, part], right_side)
    else:
        begun, others, (dual_out, log_out, out), sums = rest[0], rest[1:total], rest[total : total + 3], rest[total + 3 :]
        for m in range(total):
            block = slice(m * rows, (m + 1) * rows)
            made = begun[block, :] + dot(inverse[block, part], right_side)
            out[block, :] = made
            sums[m][...] = made if plain else made + (dual if m == n else others[m][...])
    dual_out[...] = dual
    log_out[...] = log[...]
    log_out[slot : slot + 8] += fold(gap)
    log_out[slot + 8 : slot + 16] += fold(new[...] - old[...])


def new_shares(matrix, copies, out):
    out[...] = dot(matrix[...], copies[...].astype(BF16))


def squeeze(slot, log, *rest):
    *logs, out = rest
    values = log[...]
    out[...] = jnp.sum(values.reshape(-1, 8, values.shape[-1]), axis=1)
    tail = sum(part[...] for part in logs)
    out[slot // 8 : slot // 8 + 1] += jnp.sum(tail[:8], axis=0, keepdims=True)
    out[slot // 8 + 1 : slot // 8 + 2] += jnp.sum(tail[8:], axis=0, keepdims=True)


def finish(devices, mine, got, cutoff, new, *kept):
    average = (mine[...] + got[...]) / devices
    clipped = jnp.clip(average, -cutoff[...], cutoff[...])
    new[...] = average - clipped
    for out in kept:
        out[...] = clipped


def merge(count, mine, got, log, out, log_out):
    out[...] = mine[...] + got[...]
    log_out[...] = log[...]
    log_out[:8] += fold(mine[...] - got[...]) / (2 * count)


def finish_last(devices, mine, got, kept, old, cutoff, log, new, log_out):
    mean = (mine[...] + got[...]) / devices
    average = mean + kept[...]
    made = average - jnp.clip(average, -cutoff[...], cutoff[...])
    new[...] = made
    share = devices / 2
    log_out[:8] = log[:8] + fold(mine[...] - got[...]) / (2 * devices) + share * fold(mean - made)
    log_out[8:] = log[8:] + share * fold(made - old[...])


def reduce_block(part, order, index, size, log=None):
    for step, bit in enumerate(order[:-1]):
        low, high = jnp.split(part, 2, axis=0)
        upper = (index & bit) != 0
        got = swap(jnp.where(upper, low, high), "rows", size, bit)
        mine = jnp.where(upper, high, low)
        if log is None:
            part = mine + got
        else:
            part, log = call(functools.partial(merge, 2**step), [(mine.shape, F32), (log.shape, F32)], mine, got, log)
    return part, swap(part, "rows", size, order[-1]), log


def gather_block(part, order, index, size):
    for bit in reversed(order[:-1]):
        got = swap(part, "rows", size, bit)
        upper = (index & bit) != 0
        part = jnp.concatenate([jnp.where(upper, got, part), jnp.where(upper, part, got)], axis=0)
    return part


def local(matrix, inverse, target, penalty, consensus, copy_duals, fit_parts, fit_mean, fit_duals):
    row_devices = lax.axis_size("rows")
    col_devices = lax.axis_size("cols")
    index = lax.axis_index("rows")
    block_width, targets = consensus.shape
    height = matrix.shape[0]
    normalizer = float(row_devices * col_devices * block_width * targets)
    threshold = penalty / row_devices
    row_bits = bits_of(row_devices)
    turned = row_bits[1:2] + row_bits[:1] + row_bits[2:]
    orders = [row_bits if n % 2 == 0 else turned for n in range(STREAMS)]
    rows = block_width // STREAMS
    wide, tile, piece = (block_width, targets), (height, targets), (rows, targets)
    tall = matrix.T
    shares = fit_parts[0]
    row_dual = fit_duals
    log = jnp.zeros((16 * ITERS, targets), F32)
    log_shape = (log.shape, F32)
    big = 2 * block_width * block_width * targets
    small = 2 * block_width * height * targets

    total = butterfly(shares, "cols", col_devices)
    (pulled,) = call(
        functools.partial(first_offsets, col_devices),
        [(wide, F32)], shares, total, fit_mean, row_dual, tall, flops=small,
    )
    copies, *sums = call(
        first_copies, [(wide, F32)] + [(piece, F32)] * STREAMS,
        inverse, consensus, copy_duals[0], pulled, flops=big,
    )
    centers = jnp.split(consensus, STREAMS, axis=0)
    duals = jnp.split(copy_duals[0], STREAMS, axis=0)
    owned, kept = [None] * STREAMS, [None] * STREAMS
    cutoff = threshold[None, :]
    for iteration in range(ITERS):
        slot = 16 * iteration
        last = iteration + 1 == ITERS
        plain = iteration + 2 == ITERS
        (shares,) = call(new_shares, [(tile, F32)], matrix, copies, flops=small)
        total = butterfly(shares, "cols", col_devices)
        if last:
            fitted, log = call(
                functools.partial(last_fit, col_devices, slot),
                [(tile, F32), log_shape], total, target, row_dual, log,
            )
        else:
            pulled, row_dual, log = call(
                functools.partial(next_offsets, col_devices, slot),
                [(wide, F32), (tile, F32), log_shape],
                shares, total, target, row_dual, tall, log, flops=small,
            )
        parts, logs = [], []
        for n, order in enumerate(orders):
            mine, got, tail = reduce_block(
                sums[n], order, index, row_devices, jnp.zeros((16, targets), F32) if last else None
            )
            shape = (mine.shape, F32)
            if last:
                owned[n], tail = call(
                    functools.partial(finish_last, row_devices), [shape, (tail.shape, F32)],
                    mine, got, kept[n], owned[n], cutoff, tail,
                )
                logs.append(tail)
            else:
                made = call(
                    functools.partial(finish, row_devices), [shape] * (2 if plain else 1), mine, got, cutoff
                )
                owned[n], kept[n] = made[0], made[-1]
            parts.append(gather_block(owned[n], order, index, row_devices))
        if last:
            (history,) = call(functools.partial(squeeze, slot), [((2 * ITERS, targets), F32)], log, *logs)
            centers = parts
            break
        begun = []
        for n in range(STREAMS):
            final = n == STREAMS - 1
            made = call(
                functools.partial(update, n, slot, STREAMS, plain),
                [(piece, F32), log_shape, (wide, F32)] + [(piece, F32)] * (STREAMS if final else 0),
                inverse, parts[n], centers[n], copies, duals[n], pulled, log, *begun,
                *(duals[:-1] if final else []), flops=big // STREAMS,
            )
            duals[n], log, begun = made[0], made[1], [made[2]]
            sums = made[3:]
        centers = parts
        copies = begun[0]
    history = butterfly(butterfly(history, "cols", col_devices), "rows", row_devices)
    history = (jnp.sum(history, axis=1) / normalizer).reshape(ITERS, 2)
    return (jnp.concatenate(centers, axis=0), fitted, history)


def solution(mesh):
    in_specs = (
        P("rows", "cols"),
        P("rows", "cols"),
        P("rows", None),
        P(),
        P("cols", None),
        P("rows", "cols", None),
        P("cols", "rows", None),
        P("rows", None),
        P("rows", None),
    )
    out_specs = (P("cols", None), P("rows", None), P())
    return jax.shard_map(local, mesh=mesh, in_specs=in_specs, out_specs=out_specs, check_vma=False)
```

```python
import functools

import jax
import jax.numpy as jnp
from jax import lax
from jax.experimental import pallas as pl
from jax.experimental.pallas import tpu as pltpu
from jax.sharding import PartitionSpec as P


ITERS = 5
STREAMS = 4
MERGED = 2
F32 = jnp.float32
BF16 = jnp.bfloat16


def bits_of(size):
    bits, bit = [], 1
    while bit < size:
        bits.append(bit)
        bit *= 2
    return bits


def swap(values, axis, size, bit):
    return lax.ppermute(values, axis, [(i, i ^ bit) for i in range(size)])


def butterfly(values, axis, size):
    for bit in bits_of(size):
        values = values + swap(values, axis, size, bit)
    return values


def fold(values):
    squares = values * values
    return jnp.sum(squares.reshape(-1, 8, squares.shape[-1]), axis=0)


def dot(a, b):
    return jnp.dot(a, b, preferred_element_type=F32)


def call(body, outs, *args, scratch=(), flops=0):
    return pl.pallas_call(
        body,
        out_shape=[jax.ShapeDtypeStruct(s, d) for s, d in outs],
        scratch_shapes=list(scratch),
        cost_estimate=pl.CostEstimate(flops=flops * 8, bytes_accessed=0, transcendentals=0),
        compiler_params=pltpu.CompilerParams(vmem_limit_bytes=8 * 1024 * 1024),
    )(*args)


def stage(inverse, out, sem):
    copy = pltpu.make_async_copy(inverse, out, sem)
    copy.start()
    copy.wait()


def first_offsets(cols, base, total, tall, out):
    offsets = base[...] - total[...] / cols
    out[...] = dot(tall[...], offsets.astype(BF16))


def next_offsets(cols, slot, shares, total, target, row_dual, tall, log, out, dual_out, log_out):
    mean_share = total[...] / cols
    fitted_mean = (target[...] + row_dual[...] + mean_share) / (cols + 1)
    dual = row_dual[...] + mean_share - fitted_mean
    offsets = shares[...] - mean_share + fitted_mean - dual
    out[...] = dot(tall[...], offsets.astype(BF16))
    dual_out[...] = dual
    log_out[...] = log[...]
    log_out[slot : slot + 8] += fold(mean_share - fitted_mean)


def last_fit(cols, slot, total, target, row_dual, log, out, log_out):
    mean_share = total[...] / cols
    fitted_mean = (target[...] + row_dual[...] + mean_share) / (cols + 1)
    out[...] = fitted_mean * cols
    log_out[...] = log[...]
    log_out[slot : slot + 8] += fold(mean_share - fitted_mean)


def first_copies(inverse, pulled, center, copy_dual, copies, *rest):
    *sums, right_side = rest
    right_side[...] = (center[...] - copy_dual[...] + pulled[...]).astype(BF16)
    rows = center.shape[0] // len(sums)
    for n, out in enumerate(sums):
        part = slice(n * rows, (n + 1) * rows)
        made = dot(inverse[part, :], right_side[...])
        copies[part, :] = made
        out[...] = made + copy_dual[part, :]


def block_of(ref, n, rows):
    return ref[...] if ref.shape[0] == rows else ref[n * rows : (n + 1) * rows, :]


def update(n, slot, total, plain, inverse, new, old, copies, copy_dual, pulled, log, *rest):
    rows = new.shape[0]
    part = slice(n * rows, (n + 1) * rows)
    gap = copies[part, :] - new[...]
    dual = block_of(copy_dual, n, rows) + gap
    right_side = (new[...] - dual + pulled[part, :]).astype(BF16)
    if n == 0:
        dual_out, log_out, out = rest
        out[...] = dot(inverse[:, part], right_side)
    elif n < total - 1:
        begun, dual_out, log_out, out = rest
        out[...] = begun[...] + dot(inverse[:, part], right_side)
    else:
        begun, others, (dual_out, log_out, out), sums = rest[0], rest[1:total], rest[total : total + 3], rest[total + 3 :]
        for m in range(total):
            block = slice(m * rows, (m + 1) * rows)
            made = begun[block, :] + dot(inverse[block, part], right_side)
            out[block, :] = made
            sums[m][...] = made if plain else made + (dual if m == n else others[m][...])
    dual_out[...] = dual
    log_out[...] = log[...]
    log_out[slot : slot + 8] += fold(gap)
    log_out[slot + 8 : slot + 16] += fold(new[...] - block_of(old, n, rows))


def new_shares(matrix, copies, out):
    out[...] = dot(matrix[...], copies[...].astype(BF16))


def squeeze(slot, log, *rest):
    *logs, out = rest
    values = log[...]
    out[...] = jnp.sum(values.reshape(-1, 8, values.shape[-1]), axis=1)
    tail = sum(part[...] for part in logs)
    out[slot // 8 : slot // 8 + 1] += jnp.sum(tail[:8], axis=0, keepdims=True)


def squeeze_last(slot, mine, got, *rest):
    *logs, out = rest
    tail = sum(part[...] for part in logs)
    out[...] = mine[...] + got[...]
    out[slot // 8 : slot // 8 + 1] += jnp.sum(tail[:8], axis=0, keepdims=True)
    out[slot // 8 + 1 : slot // 8 + 2] += jnp.sum(tail[8:], axis=0, keepdims=True)


def finish(devices, mine, got, cutoff, new, *kept):
    average = (mine[...] + got[...]) / devices
    clipped = jnp.clip(average, -cutoff[...], cutoff[...])
    new[...] = average - clipped
    for out in kept:
        out[...] = clipped


def merge(count, mine, got, log, out, log_out):
    out[...] = mine[...] + got[...]
    log_out[...] = log[...]
    log_out[...] += fold(mine[...] - got[...]) / (2 * count)


def finish_last(devices, mine, got, kept, old, cutoff, new, log_out):
    mean = (mine[...] + got[...]) / devices
    average = mean + kept[...]
    made = average - jnp.clip(average, -cutoff[...], cutoff[...])
    new[...] = made
    log_out[:8] = fold(mine[...] - got[...]) / devices + devices * fold(mean - made)
    log_out[8:] = devices * fold(made - old[...])


def reduce_block(part, order, index, size, log=None):
    for step, bit in enumerate(order[:-1]):
        low, high = jnp.split(part, 2, axis=0)
        upper = (index & bit) != 0
        got = swap(jnp.where(upper, low, high), "rows", size, bit)
        mine = jnp.where(upper, high, low)
        if log is None:
            part = mine + got
        else:
            part, log = call(
                functools.partial(merge, 2**step), [(mine.shape, F32), (log.shape, F32)], mine, got, log
            )
    return part, log


def gather_block(part, order, index, size):
    steps = order[-2::-1]
    for bit in steps:
        got = swap(part, "rows", size, bit)
        upper = (index & bit) != 0
        part = jnp.concatenate([jnp.where(upper, got, part), jnp.where(upper, part, got)], axis=0)
    return part


def trade_history(history, col_devices, row_devices):
    steps = [("cols", col_devices, bit) for bit in bits_of(col_devices)]
    steps += [("rows", row_devices, bit) for bit in bits_of(row_devices)[:-1]]
    for axis, size, bit in steps:
        got = swap(history, axis, size, bit)
        history = history + got
    return history


def local(matrix, inverse, target, penalty, consensus, copy_duals, fit_parts, fit_mean, fit_duals):
    row_devices = lax.axis_size("rows")
    col_devices = lax.axis_size("cols")
    index = lax.axis_index("rows")
    block_width, targets = consensus.shape
    height = matrix.shape[0]
    normalizer = float(row_devices * col_devices * block_width * targets)
    threshold = penalty / row_devices
    row_bits = bits_of(row_devices)
    turned = row_bits[1:2] + row_bits[:1] + row_bits[2:]
    orders = [row_bits if n % 2 == 0 else turned for n in range(STREAMS)]
    rows = block_width // STREAMS
    wide, tile, piece = (block_width, targets), (height, targets), (rows, targets)
    row_dual = fit_duals
    log = jnp.zeros((16 * ITERS, targets), F32)
    log_shape = (log.shape, F32)
    big = 2 * block_width * block_width * targets
    small = 2 * block_width * height * targets
    tall = matrix.T
    shares = fit_parts[0]
    total = shares + swap(shares, "cols", col_devices, 1)
    base = shares + (fit_mean - row_dual)
    for bit in bits_of(col_devices)[1:]:
        got = swap(total, "cols", col_devices, bit)
        total = total + got
    inverse = pl.pallas_call(
        stage,
        in_specs=[pl.BlockSpec(memory_space=pltpu.HBM)],
        out_shape=jax.ShapeDtypeStruct(inverse.shape, inverse.dtype),
        scratch_shapes=[pltpu.SemaphoreType.DMA],
        compiler_params=pltpu.CompilerParams(vmem_limit_bytes=40 * 1024 * 1024),
    )(inverse)
    centers, duals = [consensus] * STREAMS, [copy_duals[0]] * STREAMS
    (pulled,) = call(
        functools.partial(first_offsets, col_devices), [(wide, F32)], base, total, tall, flops=small
    )
    copies, *sums = call(
        first_copies, [(wide, F32)] + [(piece, F32)] * STREAMS, inverse, pulled, consensus, copy_duals[0],
        scratch=[pltpu.VMEM(wide, BF16)], flops=big,
    )
    owned, kept = [None] * STREAMS, [None] * STREAMS
    cutoff = threshold[None, :]
    for iteration in range(ITERS):
        slot = 16 * iteration
        last = iteration + 1 == ITERS
        plain = iteration + 2 == ITERS
        (shares,) = call(new_shares, [(tile, F32)], matrix, copies, flops=small)
        total = butterfly(shares, "cols", col_devices)
        if last:
            fitted, log = call(
                functools.partial(last_fit, col_devices, slot),
                [(tile, F32), log_shape], total, target, row_dual, log,
            )
        else:
            pulled, row_dual, log = call(
                functools.partial(next_offsets, col_devices, slot),
                [(wide, F32), (tile, F32), log_shape],
                shares, total, target, row_dual, tall, log, flops=small,
            )
        pairs = [
            reduce_block(sums[n], order, index, row_devices, jnp.zeros((8, targets), F32) if last else None)
            for n, order in enumerate(orders)
        ]
        partner = row_bits[-1]
        if last:
            (history,) = call(
                functools.partial(squeeze, slot), [((2 * ITERS, targets), F32)], log,
                *[pair[1] for pair in pairs],
            )
            early = swap(history, "rows", row_devices, partner)
        parts, logs = [], []
        for first in range(0, STREAMS, MERGED):
            group = range(first, first + MERGED)
            joined = jnp.concatenate([pairs[n][0] for n in group], axis=0)
            traded = swap(joined, "rows", row_devices, partner)
            traded = jnp.split(traded, MERGED, axis=0)
            for n, got in zip(group, traded):
                mine = pairs[n][0]
                shape = (mine.shape, F32)
                if last:
                    owned[n], tail = call(
                        functools.partial(finish_last, row_devices), [shape, ((16, targets), F32)],
                        mine, got, kept[n], owned[n], cutoff,
                    )
                    logs.append(tail)
                else:
                    made = call(
                        functools.partial(finish, row_devices), [shape] * (2 if plain else 1), mine, got, cutoff
                    )
                    owned[n], kept[n] = made[0], made[-1]
                parts.append(gather_block(owned[n], orders[n], index, row_devices))
        if last:
            (history,) = call(
                functools.partial(squeeze_last, slot), [((2 * ITERS, targets), F32)], history, early, *logs
            )
            history = trade_history(history, col_devices, row_devices)
            centers = parts
            break
        begun = []
        for n in range(STREAMS):
            final = n == STREAMS - 1
            made = call(
                functools.partial(update, n, slot, STREAMS, plain),
                [(piece, F32), log_shape, (wide, F32)] + [(piece, F32)] * (STREAMS if final else 0),
                inverse, parts[n], centers[n], copies, duals[n], pulled, log, *begun,
                *(duals[:-1] if final else []), flops=big // STREAMS,
            )
            duals[n], log, begun = made[0], made[1], [made[2]]
            sums = made[3:]
        centers = parts
        copies = begun[0]
    history = (jnp.sum(history, axis=1) / normalizer).reshape(ITERS, 2)
    return (jnp.concatenate(centers, axis=0), fitted, history)


def solution(mesh):
    in_specs = (
        P("rows", "cols"),
        P("rows", "cols"),
        P("rows", None),
        P(),
        P("cols", None),
        P("rows", "cols", None),
        P("cols", "rows", None),
        P("rows", None),
        P("rows", None),
    )
    out_specs = (P("cols", None), P("rows", None), P())
    return jax.shard_map(local, mesh=mesh, in_specs=in_specs, out_specs=out_specs, check_vma=False)
```

```python
import functools

import jax
import jax.numpy as jnp
from jax import lax
from jax.experimental import pallas as pl
from jax.experimental.pallas import tpu as pltpu
from jax.sharding import PartitionSpec as P


ITERS = 5
STREAMS = 4
MERGED = 2
F32 = jnp.float32
BF16 = jnp.bfloat16


def bits_of(size):
    bits, bit = [], 1
    while bit < size:
        bits.append(bit)
        bit *= 2
    return bits


def swap(values, axis, size, bit):
    return lax.ppermute(values, axis, [(i, i ^ bit) for i in range(size)])


def fold(values):
    squares = values * values
    return jnp.sum(squares.reshape(-1, 8, squares.shape[-1]), axis=0)


def dot(a, b):
    return jnp.dot(a, b, preferred_element_type=F32)


def call(body, outs, *args, scratch=(), flops=0):
    return pl.pallas_call(
        body,
        out_shape=[jax.ShapeDtypeStruct(s, d) for s, d in outs],
        scratch_shapes=list(scratch),
        cost_estimate=pl.CostEstimate(flops=flops * 8, bytes_accessed=0, transcendentals=0),
        compiler_params=pltpu.CompilerParams(vmem_limit_bytes=8 * 1024 * 1024),
    )(*args)


def stage(inverse, out, sem):
    copy = pltpu.make_async_copy(inverse, out, sem)
    copy.start()
    copy.wait()


def first_offsets(cols, base, total, tall, out):
    offsets = base[...] - total[...] / cols
    out[...] = dot(tall[...], offsets.astype(BF16))


def next_offsets(cols, slot, shares, total, target, row_dual, tall, log, out, dual_out, log_out):
    mean_share = total[...] / cols
    fitted_mean = (target[...] + row_dual[...] + mean_share) / (cols + 1)
    dual = row_dual[...] + mean_share - fitted_mean
    offsets = shares[...] - mean_share + fitted_mean - dual
    out[...] = dot(tall[...], offsets.astype(BF16))
    dual_out[...] = dual
    log_out[...] = log[...]
    log_out[slot : slot + 8] += fold(mean_share - fitted_mean)


def last_fit(cols, slot, total, target, row_dual, log, out, log_out):
    mean_share = total[...] / cols
    fitted_mean = (target[...] + row_dual[...] + mean_share) / (cols + 1)
    out[...] = fitted_mean * cols
    log_out[...] = log[...]
    log_out[slot : slot + 8] += fold(mean_share - fitted_mean)


def first_copies(inverse, pulled, center, copy_dual, copies, *rest):
    *sums, right_side = rest
    right_side[...] = (center[...] - copy_dual[...] + pulled[...]).astype(BF16)
    rows = center.shape[0] // len(sums)
    for n, out in enumerate(sums):
        part = slice(n * rows, (n + 1) * rows)
        made = dot(inverse[part, :], right_side[...])
        copies[part, :] = made
        out[...] = made + copy_dual[part, :]


def block_of(ref, n, rows):
    return ref[...] if ref.shape[0] == rows else ref[n * rows : (n + 1) * rows, :]


def update(n, slot, total, plain, inverse, new, old, copies, copy_dual, pulled, log, *rest):
    rows = new.shape[0]
    part = slice(n * rows, (n + 1) * rows)
    gap = copies[part, :] - new[...]
    dual = block_of(copy_dual, n, rows) + gap
    right_side = (new[...] - dual + pulled[part, :]).astype(BF16)
    if n == 0:
        dual_out, log_out, out = rest
        out[...] = dot(inverse[:, part], right_side)
    elif n < total - 1:
        begun, dual_out, log_out, out = rest
        out[...] = begun[...] + dot(inverse[:, part], right_side)
    else:
        begun, others, (dual_out, log_out, out), sums = rest[0], rest[1:total], rest[total : total + 3], rest[total + 3 :]
        for m in range(total):
            block = slice(m * rows, (m + 1) * rows)
            made = begun[block, :] + dot(inverse[block, part], right_side)
            out[block, :] = made
            sums[m][...] = made if plain else made + (dual if m == n else others[m][...])
    dual_out[...] = dual
    log_out[...] = log[...]
    log_out[slot : slot + 8] += fold(gap)
    log_out[slot + 8 : slot + 16] += fold(new[...] - block_of(old, n, rows))


def new_shares(matrix, copies, out):
    out[...] = dot(matrix[...], copies[...].astype(BF16))


def squeeze(slot, log, *rest):
    *logs, out = rest
    values = log[...]
    out[...] = jnp.sum(values.reshape(-1, 8, values.shape[-1]), axis=1)
    tail = sum(part[...] for part in logs)
    out[slot // 8 : slot // 8 + 1] += jnp.sum(tail[:8], axis=0, keepdims=True)


def squeeze_last(slot, mine, got, *rest):
    *logs, out = rest
    tail = sum(part[...] for part in logs)
    out[...] = mine[...] + got[...]
    out[slot // 8 : slot // 8 + 1] += jnp.sum(tail[:8], axis=0, keepdims=True)
    out[slot // 8 + 1 : slot // 8 + 2] += jnp.sum(tail[8:], axis=0, keepdims=True)


def finish(devices, mine, got, cutoff, new, *kept):
    average = (mine[...] + got[...]) / devices
    clipped = jnp.clip(average, -cutoff[...], cutoff[...])
    new[...] = average - clipped
    for out in kept:
        out[...] = clipped


def merge(count, mine, got, log, out, log_out):
    out[...] = mine[...] + got[...]
    log_out[...] = log[...]
    log_out[...] += fold(mine[...] - got[...]) / (2 * count)


def finish_last(devices, mine, got, kept, old, cutoff, new, log_out):
    mean = (mine[...] + got[...]) / devices
    average = mean + kept[...]
    made = average - jnp.clip(average, -cutoff[...], cutoff[...])
    new[...] = made
    log_out[:8] = fold(mine[...] - got[...]) / devices + devices * fold(mean - made)
    log_out[8:] = devices * fold(made - old[...])


def reduce_block(part, order, index, size, log=None):
    for step, bit in enumerate(order[:-1]):
        low, high = jnp.split(part, 2, axis=0)
        upper = (index & bit) != 0
        got = swap(jnp.where(upper, low, high), "rows", size, bit)
        mine = jnp.where(upper, high, low)
        if log is None:
            part = mine + got
        else:
            part, log = call(
                functools.partial(merge, 2**step), [(mine.shape, F32), (log.shape, F32)], mine, got, log
            )
    return part, log


def gather_block(part, order, index, size):
    steps = order[-2::-1]
    for bit in steps:
        got = swap(part, "rows", size, bit)
        upper = (index & bit) != 0
        part = jnp.concatenate([jnp.where(upper, got, part), jnp.where(upper, part, got)], axis=0)
    return part


def trade_history(history, col_devices, row_devices):
    steps = [("cols", col_devices, bit) for bit in bits_of(col_devices)]
    steps += [("rows", row_devices, bit) for bit in bits_of(row_devices)[:-1]]
    for axis, size, bit in steps:
        got = swap(history, axis, size, bit)
        history = history + got
    return history


def local(matrix, inverse, target, penalty, consensus, copy_duals, fit_parts, fit_mean, fit_duals):
    row_devices = lax.axis_size("rows")
    col_devices = lax.axis_size("cols")
    index = lax.axis_index("rows")
    block_width, targets = consensus.shape
    height = matrix.shape[0]
    normalizer = float(row_devices * col_devices * block_width * targets)
    threshold = penalty / row_devices
    row_bits = bits_of(row_devices)
    turned = row_bits[1:2] + row_bits[:1] + row_bits[2:]
    orders = [row_bits if n % 2 == 0 else turned for n in range(STREAMS)]
    rows = block_width // STREAMS
    wide, tile, piece = (block_width, targets), (height, targets), (rows, targets)
    row_dual = fit_duals
    log = jnp.zeros((16 * ITERS, targets), F32)
    log_shape = (log.shape, F32)
    big = 2 * block_width * block_width * targets
    small = 2 * block_width * height * targets
    tall = matrix.T
    shares = fit_parts[0]
    total = shares + swap(shares, "cols", col_devices, 1)
    base = shares + (fit_mean - row_dual)
    for bit in bits_of(col_devices)[1:]:
        got = swap(total, "cols", col_devices, bit)
        total = total + got
    inverse = pl.pallas_call(
        stage,
        in_specs=[pl.BlockSpec(memory_space=pltpu.HBM)],
        out_shape=jax.ShapeDtypeStruct(inverse.shape, inverse.dtype),
        scratch_shapes=[pltpu.SemaphoreType.DMA],
        compiler_params=pltpu.CompilerParams(vmem_limit_bytes=40 * 1024 * 1024),
    )(inverse)
    centers, duals = [consensus] * STREAMS, [copy_duals[0]] * STREAMS
    (pulled,) = call(
        functools.partial(first_offsets, col_devices), [(wide, F32)], base, total, tall, flops=small
    )
    copies, *sums = call(
        first_copies, [(wide, F32)] + [(piece, F32)] * STREAMS, inverse, pulled, consensus, copy_duals[0],
        scratch=[pltpu.VMEM(wide, BF16)], flops=big,
    )
    owned, kept = [None] * STREAMS, [None] * STREAMS
    cutoff = threshold[None, :]
    for iteration in range(ITERS):
        slot = 16 * iteration
        last = iteration + 1 == ITERS
        plain = iteration + 2 == ITERS
        (shares,) = call(new_shares, [(tile, F32)], matrix, copies, flops=small)
        total = shares
        for bit in bits_of(col_devices):
            got = swap(total, "cols", col_devices, bit)
            total = total + got
        if last:
            fitted, log = call(
                functools.partial(last_fit, col_devices, slot),
                [(tile, F32), log_shape], total, target, row_dual, log,
            )
        else:
            pulled, row_dual, log = call(
                functools.partial(next_offsets, col_devices, slot),
                [(wide, F32), (tile, F32), log_shape],
                shares, total, target, row_dual, tall, log, flops=small,
            )
        pairs = [
            reduce_block(sums[n], order, index, row_devices, jnp.zeros((8, targets), F32) if last else None)
            for n, order in enumerate(orders)
        ]
        partner = row_bits[-1]
        if last:
            (history,) = call(
                functools.partial(squeeze, slot), [((2 * ITERS, targets), F32)], log,
                *[pair[1] for pair in pairs],
            )
            early = swap(history, "rows", row_devices, partner)
        parts, logs = [], []
        for first in range(0, STREAMS, MERGED):
            group = range(first, first + MERGED)
            joined = jnp.concatenate([pairs[n][0] for n in group], axis=0)
            traded = swap(joined, "rows", row_devices, partner)
            traded = jnp.split(traded, MERGED, axis=0)
            for n, got in zip(group, traded):
                mine = pairs[n][0]
                shape = (mine.shape, F32)
                if last:
                    owned[n], tail = call(
                        functools.partial(finish_last, row_devices), [shape, ((16, targets), F32)],
                        mine, got, kept[n], owned[n], cutoff,
                    )
                    logs.append(tail)
                else:
                    made = call(
                        functools.partial(finish, row_devices), [shape] * (2 if plain else 1), mine, got, cutoff
                    )
                    owned[n], kept[n] = made[0], made[-1]
                parts.append(gather_block(owned[n], orders[n], index, row_devices))
        if last:
            (history,) = call(
                functools.partial(squeeze_last, slot), [((2 * ITERS, targets), F32)], history, early, *logs
            )
            history = trade_history(history, col_devices, row_devices)
            centers = parts
            break
        begun = []
        for n in range(STREAMS):
            final = n == STREAMS - 1
            made = call(
                functools.partial(update, n, slot, STREAMS, plain),
                [(piece, F32), log_shape, (wide, F32)] + [(piece, F32)] * (STREAMS if final else 0),
                inverse, parts[n], centers[n], copies, duals[n], pulled, log, *begun,
                *(duals[:-1] if final else []), flops=big // STREAMS,
            )
            duals[n], log, begun = made[0], made[1], [made[2]]
            sums = made[3:]
        centers = parts
        copies = begun[0]
    history = (jnp.sum(history, axis=1) / normalizer).reshape(ITERS, 2)
    return (jnp.concatenate(centers, axis=0), fitted, history)


def solution(mesh):
    in_specs = (
        P("rows", "cols"),
        P("rows", "cols"),
        P("rows", None),
        P(),
        P("cols", None),
        P("rows", "cols", None),
        P("cols", "rows", None),
        P("rows", None),
        P("rows", None),
    )
    out_specs = (P("cols", None), P("rows", None), P())
    return jax.shard_map(local, mesh=mesh, in_specs=in_specs, out_specs=out_specs, check_vma=False)
```
